32 devices in a mesh: gx: 4 (over y, core), gy: 2 (over x), gz: 4 (over z).
Axes of the slice: x: 2, y: 2, z: 4, core: 2. Of those that a mesh axis runs over, the one named last changes fastest.
Arguments:
- positions: float32 [3, 4096, 128], P(None, ('gx', 'gy', 'gz')), may hold values from 0 to 1, as said below
- charges: float32 [4096, 128], P(('gx', 'gy', 'gz')), may hold values from -6 to 6
- velocities: float32 [3, 4096, 128], P(None, ('gx', 'gy', 'gz')), may hold values from -6 to 6
- leaf_ids: int32 [4096], P(('gx', 'gy', 'gz')), may hold values from 0 to 2097151, as said below
- live_counts: int32 [32], replicated, may hold values from 32 to 96
- send_counts: int32 [5, 32], replicated, may hold values from 0 to 32, as said below
Outputs:
- moved_positions: float32 [3, 4096, 128], P(None, ('gx', 'gy', 'gz'))
- moved_charges: float32 [4096, 128], P(('gx', 'gy', 'gz'))
- moved_velocities: float32 [3, 4096, 128], P(None, ('gx', 'gy', 'gz'))
- moved_leaves: int32 [4096], P(('gx', 'gy', 'gz'))
- leaf_moments: float32 [286, 4096], P(None, ('gx', 'gy', 'gz'))
- parent_moments: float32 [286, 4096], P(None, ('gx', 'gy', 'gz'))
The draws below stay inside these ranges and needn't reach their ends.
Inputs may be any that keep to these rules, and one draw needn't show every extreme that they name: `positions`: every particle of a live slot lies inside the leaf cell of side 2^-7 named by the slot's leaf index. `leaf_ids`: morton indices of cells at depth 7; a leaf's parent cell is its index // 8. `send_counts`: no device sends more blocks than it holds live; after every section no device holds more than 128 live blocks; in every draw some device sends exactly 32 blocks in the first section and its partner then holds exactly 128.
All inputs are finite; a program needn't handle non-finite values.
Results may differ from the reference program's by a relative error of at most 0.0003.
Values sent between devices are 32-bit elements; how exact they have to be, the bound alone decides.
A program may use at most 128 MiB of HBM per device.

```python
import math
from functools import partial
import jax
import jax.numpy as jnp
import numpy as np
from jax import lax

CAP = 128
PART = 128
ORDER = 10
LEVEL = 7
SEND_CAP = 32
SECTIONS = 5
NCOEF = 286
BLOCKS = 4096
N_GX = 4
N_GY = 2
DEVICES = 32


def leaf_table(key):
    base_key = jax.random.fold_in(key, 11)
    climb_key, start_key, octant_key, order_key = jax.random.split(base_key, 4)
    climbs = (jax.random.randint(climb_key, (DEVICES, CAP), 0, 3) == 0).astype(jnp.int32)
    parents = jax.random.randint(start_key, (DEVICES, 1), 0, 8 ** (LEVEL - 1) - CAP) + jnp.cumsum(climbs, axis=1)
    row_keys = jax.random.split(order_key, DEVICES)
    parents = jax.vmap(jax.random.permutation)(row_keys, parents)
    octants = jax.random.randint(octant_key, (DEVICES, CAP), 0, 8)
    return (parents * 8 + octants).reshape(DEVICES * CAP).astype(jnp.int32)


def route_plan(key):
    base_key = jax.random.fold_in(key, 37)
    start_key, pair_key, section_key = jax.random.split(base_key, 3)
    quarter = CAP // 4
    live_now = jax.random.randint(start_key, (DEVICES,), quarter, 3 * quarter + 1)
    half_way = DEVICES // 2
    chosen = jax.random.randint(pair_key, (), 0, half_way)
    live_now = live_now.at[chosen].set(3 * quarter).at[chosen + half_way].set(3 * quarter)
    initial = live_now
    everyone = jnp.arange(DEVICES, dtype=jnp.int32)
    outer_bits = int(N_GX).bit_length() - 1
    middle_bits = int(N_GY).bit_length() - 1
    phase_firsts = [0, outer_bits, outer_bits + middle_bits]
    sender = chosen.astype(jnp.int32)
    holder = (chosen + half_way).astype(jnp.int32)
    count_rows = []
    for section_num in range(SECTIONS):
        bit_mask = 1 << SECTIONS - 1 - section_num
        partner = jnp.bitwise_xor(everyone, bit_mask)
        lower_half = jnp.bitwise_and(everyone, bit_mask) == 0
        phase_start = section_num in phase_firsts
        if phase_start and section_num > 0:
            sender = jnp.argmax(live_now).astype(jnp.int32)
            holder = jnp.bitwise_xor(sender, bit_mask)
        is_sender = everyone == sender
        is_holder = everyone == holder
        low_key, high_key = jax.random.split(jax.random.fold_in(section_key, section_num))
        low_count = jax.random.randint(low_key, (DEVICES,), 0, jnp.minimum(live_now, SEND_CAP) + 1)
        if phase_start:
            low_count = jnp.where(is_sender, SEND_CAP, low_count)
            low_count = jnp.where(is_holder, jnp.maximum(low_count, live_now + SEND_CAP - CAP), low_count)
        else:
            spare_room = CAP - live_now[holder]
            low_count = jnp.where(is_holder, 0, low_count)
            low_count = jnp.where(partner == holder, jnp.minimum(low_count, spare_room), low_count)
        paired_count = low_count[partner]
        held_count = live_now[partner]
        lowest = jnp.maximum(0, live_now + paired_count - CAP)
        highest = jnp.maximum(lowest, jnp.minimum(jnp.minimum(live_now, SEND_CAP), CAP - held_count + paired_count))
        high_count = jax.random.randint(high_key, (DEVICES,), lowest, highest + 1)
        if phase_start:
            high_count = jnp.where(is_sender, SEND_CAP, high_count)
        else:
            high_count = jnp.where(is_holder, 0, high_count)
        if section_num == 0:
            high_count = jnp.where(is_holder, 0, high_count)
        counts = jnp.where(lower_half, low_count, high_count)
        count_rows.append(counts)
        live_now = live_now - counts + counts[partner]
    return (initial.astype(jnp.int32), jnp.stack(count_rows).astype(jnp.int32))


def draw_leaf_ids(key, part):
    return leaf_table(key)


def draw_live_counts(key, part):
    return route_plan(key)[0]


def draw_send_counts(key, part):
    return route_plan(key)[1]


def draw_positions(key, part):
    leaves = leaf_table(key)
    coordinates = []
    for axis_bit in (2, 1, 0):
        coordinate = jnp.zeros_like(leaves)
        for level_num in range(LEVEL):
            octant_id = jnp.right_shift(leaves, 3 * level_num)
            coordinate = coordinate + jnp.left_shift(jnp.bitwise_and(jnp.right_shift(octant_id, axis_bit), 1), level_num)
        coordinates.append(coordinate.astype(jnp.float32))
    cell_grid = jnp.stack(coordinates)
    fraction = jax.random.uniform(jax.random.fold_in(key, 23), (3, DEVICES * CAP, PART), jnp.float32, 0.0, 1.0)
    fraction = 0.001 + 0.998 * fraction
    return ((cell_grid[:, :, None] + fraction) / float(2 ** LEVEL)).astype(jnp.float32)


def level_of(own_key, dims, cuts, low, largest):
    loudness, own = 1.0, jax.random.fold_in(own_key, 6)
    for axis_at, blocks in cuts:
        heights = jnp.exp(jax.random.uniform(jax.random.fold_in(own, axis_at), (blocks,), jnp.float32, low / len(cuts), largest / len(cuts)))
        loudness = loudness * jnp.repeat(heights, dims[axis_at] // blocks).reshape([-1 if axis == axis_at else 1 for axis in range(len(dims))])
    return loudness


def noise(own_key, shape, deviation, bound, cuts=(), kind=jnp.bfloat16):
    factor_of = level_of(own_key, shape, cuts, -0.22, 0.18) if cuts else 1.0
    entries = jax.random.normal(own_key, shape, jnp.float32) * deviation * factor_of
    return jnp.minimum(jnp.maximum(entries, -bound), bound).astype(kind)


def setup_inputs(seed: int = 0) -> dict:
    streams_of = jax.random.split(jax.random.key(seed), 7)
    positions = draw_positions(jax.random.fold_in(streams_of[6], 71), 0)
    charges = noise(streams_of[1], (BLOCKS, PART), 1.0, 6.0, ((0, 32),), jnp.float32)
    velocities = noise(streams_of[2], (3, BLOCKS, PART), 1.0, 6.0, ((1, 32),), jnp.float32)
    leaf_ids = draw_leaf_ids(jax.random.fold_in(streams_of[6], 71), 0)
    live_counts = draw_live_counts(jax.random.fold_in(streams_of[6], 71), 0)
    send_counts = draw_send_counts(jax.random.fold_in(streams_of[6], 71), 0)
    return dict(positions=positions, charges=charges, velocities=velocities, leaf_ids=leaf_ids, live_counts=live_counts, send_counts=send_counts)


def exponents(max_order):
    return [(p, q, r) for p in range(max_order + 1) for q in range(max_order + 1 - p) for r in range(max_order + 1 - p - q)]


def shift_tables(max_order):
    triples = exponents(max_order)
    count = len(triples)
    tables = np.zeros((8, count, count))
    for octant_id in range(8):
        signs = [0.5 if (octant_id >> shift_bit) & 1 else -0.5 for shift_bit in (2, 1, 0)]
        for k, (p, q, r) in enumerate(triples):
            for j, (e, f, g) in enumerate(triples):
                if e <= p and f <= q and g <= r:
                    tables[octant_id, k, j] = (math.comb(p, e) * math.comb(q, f) * math.comb(r, g)
                                               * signs[0] ** (p - e) * signs[1] ** (q - f) * signs[2] ** (r - g)
                                               * 0.5 ** (e + f + g))
    return jnp.asarray(tables, jnp.float32)


def morton_cells(leaves, tree_depth):
    coordinates = []
    for axis_bit in (2, 1, 0):
        coordinate = jnp.zeros_like(leaves)
        for level_num in range(tree_depth):
            octant_id = jnp.right_shift(leaves, 3 * level_num)
            coordinate = coordinate + jnp.left_shift(jnp.bitwise_and(jnp.right_shift(octant_id, axis_bit), 1), level_num)
        coordinates.append(coordinate)
    return coordinates


def leaf_moments(positions, charges, leaves, max_order, tree_depth):
    cells_side = float(2 ** tree_depth)
    coordinates = morton_cells(leaves, tree_depth)
    powers = []
    for axis_num in range(3):
        offset_row = 2.0 * (positions[axis_num] * cells_side - coordinates[axis_num].astype(jnp.float32)[:, None]) - 1.0
        power_list = [jnp.ones_like(offset_row)]
        for degree_num in range(max_order):
            power_list.append(power_list[-1] * offset_row)
        powers.append(power_list)
    exponent_pairs = [(p, q) for p in range(max_order + 1) for q in range(max_order + 1 - p)]
    weighted = jnp.stack([charges * powers[0][p] * powers[1][q] for p, q in exponent_pairs])
    third_powers = jnp.stack(powers[2])
    raw_sums = jnp.einsum('pbi,cbi->pcb', weighted, third_powers, precision=lax.Precision.HIGHEST)
    pieces = [raw_sums[n, :max_order + 1 - p - q] for n, (p, q) in enumerate(exponent_pairs)]
    return jnp.concatenate(pieces, axis=0) / 16.0


def parent_moments(moments, leaves, live_mask, tables):
    shifted = jnp.einsum('okj,jb->okb', tables, moments, precision=lax.Precision.HIGHEST)
    octant_id = jnp.bitwise_and(leaves, 7)
    chooser = (octant_id[None, :] == jnp.arange(8, dtype=jnp.int32)[:, None]).astype(jnp.float32)
    moved = jnp.sum(shifted * chooser[:, None, :], axis=0)
    parents = jnp.right_shift(leaves, 3)
    sibling = ((parents[:, None] == parents[None, :]) & live_mask[:, None] & live_mask[None, :]).astype(jnp.float32)
    return jnp.dot(moved, sibling, precision=lax.Precision.HIGHEST, preferred_element_type=jnp.float32)


def outgoing(blocks_now, live_count, sent_count, upper_half, slab_rows):
    start_at = jnp.where(upper_half, 0, live_count - sent_count).astype(jnp.int32)

    def cut(member):
        padding = jnp.zeros(member.shape[:1] + (slab_rows,) + member.shape[2:], member.dtype)
        return lax.dynamic_slice_in_dim(jnp.concatenate([member, padding], axis=1), start_at, slab_rows, 1)

    return jax.tree.map(cut, blocks_now)


def incoming(blocks_now, arrived, live_count, sent_count, got_count, upper_half):
    kept_count = live_count - sent_count

    def place(member, slab_part):
        slot_total = member.shape[1]
        slab_rows = slab_part.shape[1]
        edge_pad = jnp.zeros(member.shape[:1] + (slab_rows,) + member.shape[2:], member.dtype)
        wide_pad = jnp.zeros(member.shape, member.dtype)
        offset_old = jnp.where(upper_half, sent_count - got_count, 0)
        shifted = lax.dynamic_slice_in_dim(jnp.concatenate([edge_pad, member, edge_pad], axis=1),
                                           (slab_rows + offset_old).astype(jnp.int32), slot_total, 1)
        offset_new = jnp.where(upper_half, 0, kept_count)
        placed = lax.dynamic_slice_in_dim(jnp.concatenate([wide_pad, slab_part, wide_pad], axis=1),
                                          (slot_total - offset_new).astype(jnp.int32), slot_total, 1)
        slot_ids = jnp.arange(slot_total, dtype=jnp.int32)
        take_new = jnp.where(upper_half, slot_ids < got_count, (slot_ids >= kept_count) & (slot_ids < kept_count + got_count))
        take_old = jnp.where(upper_half, (slot_ids >= got_count) & (slot_ids < got_count + kept_count), slot_ids < kept_count)
        shape_mask = (1, slot_total) + (1,) * (member.ndim - 2)
        take_new = take_new.reshape(shape_mask)
        take_old = take_old.reshape(shape_mask)
        return jnp.where(take_new, placed, jnp.where(take_old, shifted, jnp.zeros_like(member)))

    return jax.tree.map(place, blocks_now, arrived)


def reference(positions, charges, velocities, leaf_ids, live_counts, send_counts):
    blocks_now = (jnp.moveaxis(positions.reshape(3, DEVICES, CAP, PART), 1, 0),
                  charges.reshape(DEVICES, 1, CAP, PART),
                  jnp.moveaxis(velocities.reshape(3, DEVICES, CAP, PART), 1, 0),
                  leaf_ids.astype(jnp.float32).reshape(DEVICES, 1, CAP))
    everyone = jnp.arange(DEVICES, dtype=jnp.int32)
    live_all = live_counts
    send_out = partial(outgoing, slab_rows=SEND_CAP)
    for section_num in range(SECTIONS):
        bit_mask = 1 << (SECTIONS - 1 - section_num)
        partner = jnp.bitwise_xor(everyone, bit_mask)
        upper_half = jnp.bitwise_and(everyone, bit_mask) != 0
        sent_count = send_counts[section_num]
        got_count = sent_count[partner]
        outbound = jax.vmap(send_out)(blocks_now, live_all, sent_count, upper_half)
        arrived = jax.tree.map(lambda member: member[partner], outbound)
        blocks_now = jax.vmap(incoming)(blocks_now, arrived, live_all, sent_count, got_count, upper_half)
        live_all = live_all - sent_count + got_count
    tables = shift_tables(ORDER)

    def settle(inputs):
        device_positions, device_charges, device_leaves, live_count = inputs
        live_mask = jnp.arange(CAP, dtype=jnp.int32) < live_count
        leaves = jnp.where(live_mask, device_leaves[0].astype(jnp.int32), 0)
        leaf_part = leaf_moments(device_positions, device_charges[0], leaves, ORDER, LEVEL)
        return leaf_part, parent_moments(leaf_part, leaves, live_mask, tables)

    leaf_part, parent_part = lax.map(settle, (blocks_now[0], blocks_now[1], blocks_now[3], live_all))
    all_mask = jnp.arange(CAP, dtype=jnp.int32)[None, :] < live_all[:, None]
    moved_leaves = jnp.where(all_mask, blocks_now[3][:, 0].astype(jnp.int32), -1).reshape(BLOCKS)
    moved_positions = jnp.moveaxis(blocks_now[0], 0, 1).reshape(3, BLOCKS, PART)
    moved_charges = blocks_now[1].reshape(BLOCKS, PART)
    moved_velocities = jnp.moveaxis(blocks_now[2], 0, 1).reshape(3, BLOCKS, PART)
    first_out = jnp.moveaxis(leaf_part, 0, 1).reshape(NCOEF, BLOCKS)
    second_out = jnp.moveaxis(parent_part, 0, 1).reshape(NCOEF, BLOCKS)
    return (moved_positions, moved_charges, moved_velocities, moved_leaves, first_out, second_out)
```

```python
import functools
import math

import jax
import jax.numpy as jnp
import numpy as np
from jax import lax
from jax.experimental import pallas as pl
from jax.experimental.pallas import tpu as pltpu
from jax.sharding import PartitionSpec as P

ORDER = 10
LEVEL = 7
AXES = ("gx", "gy", "gz")
TILE = 8


def exponents(max_order):
    return [
        (p, q, r)
        for p in range(max_order + 1)
        for q in range(max_order + 1 - p)
        for r in range(max_order + 1 - p - q)
    ]


def shift_constants(max_order, rows, lanes):
    triples = exponents(max_order)
    table = np.zeros((rows, rows))
    parity = np.zeros((rows, lanes), np.int32)
    for k, (p, q, r) in enumerate(triples):
        parity[k] = (p & 1) * 4 + (q & 1) * 2 + (r & 1)
        for j, (e, f, g) in enumerate(triples):
            if e <= p and f <= q and g <= r:
                ways = math.comb(p, e) * math.comb(q, f) * math.comb(r, g)
                table[k, j] = ways * 0.5 ** (p + q + r)
    return jnp.asarray(table, jnp.bfloat16), jnp.asarray(parity)


def exchange_kernel(
    sizes,
    live_ref,
    sends_ref,
    leaf_ref,
    pos_ref,
    chg_ref,
    vel_ref,
    out_ref,
    leaf_out_ref,
    state_a,
    state_b,
    send_a,
    send_b,
    in_sem,
    send_sem,
    recv_sem,
    *recv_all,
):
    nx, ny, nz = sizes
    recv_a, recv_b = recv_all[0::2], recv_all[1::2]
    sections = (nx * ny * nz).bit_length() - 1
    slots, part = chg_ref.shape
    slab = slots // 4
    pad = slab
    groups = ((state_a, send_a, recv_a, 4, 0), (state_b, send_b, recv_b, 3, 4))
    device = (lax.axis_index("gx") * ny + lax.axis_index("gy")) * nz + lax.axis_index("gz")

    loads = [
        pltpu.make_async_copy(pos_ref, state_a.at[0, 0:3, pad : pad + slots, :], in_sem.at[0]),
        pltpu.make_async_copy(chg_ref, state_a.at[0, 3, pad : pad + slots, :], in_sem.at[1]),
        pltpu.make_async_copy(vel_ref, state_b.at[0, 0:3, pad : pad + slots, :], in_sem.at[2]),
    ]
    for load in loads:
        load.start()

    masks = [1 << (sections - 1 - s) for s in range(sections)]
    uppers = [lax.rem(lax.div(device, m), 2) for m in masks]
    partners = [device + m - 2 * m * up for m, up in zip(masks, uppers)]
    places = [
        (lax.div(e, ny * nz), lax.rem(lax.div(e, nz), ny), lax.rem(e, nz)) for e in partners
    ]

    barrier = pltpu.get_barrier_semaphore()
    for place in places:
        pl.semaphore_signal(
            barrier, inc=1, device_id=place, device_id_type=pl.DeviceIdType.MESH
        )

    live = live_ref[device]
    plans = []
    for s in range(sections):
        sent = sends_ref[s, device]
        got = sends_ref[s, partners[s]]
        up = uppers[s]
        kept = live - sent
        start = (1 - up) * kept
        old_by = up * (sent - got)
        new_at = (1 - up) * kept
        plans.append((start, old_by, new_at, got))
        live = kept + got

    for state, send, recv, members, _ in groups:
        edge = jnp.zeros((members, pad, part), jnp.float32)
        for side in range(2):
            state[side, :, 0:pad, :] = edge
            state[side, :, pad + slots : 2 * pad + slots, :] = edge
        rows = TILE + members * slab
        for s in range(sections):
            recv[s][rows : rows + TILE, :] = jnp.zeros((TILE, part), jnp.float32)
    for s in range(sections):
        send_b[s, 0:TILE, :] = jnp.zeros((TILE, part), jnp.float32)

    leaf = jnp.broadcast_to(leaf_ref[...], (TILE, slots)).astype(jnp.float32)
    lane = lax.broadcasted_iota(jnp.int32, (TILE, slots), 1)
    row = lax.broadcasted_iota(jnp.int32, (TILE, part), 0)

    def copy_of(s, g):
        _, send, recv, members, _ = groups[g]
        rows = TILE + members * slab
        return pltpu.make_async_remote_copy(
            src_ref=send.at[s],
            dst_ref=recv[s].at[0:rows, :],
            send_sem=send_sem.at[s, g],
            recv_sem=recv_sem.at[s, g],
            device_id=places[s],
            device_id_type=pl.DeviceIdType.MESH,
        )

    def emit(s, g, leaf):
        state, send, _, members, _ = groups[g]
        start = plans[s][0]
        if g == 0:
            send[s, 0:TILE, :] = pltpu.roll(leaf, lax.rem(slots - start, slots), 1)
        for m in range(members):
            at = TILE + m * slab
            send[s, at : at + slab, :] = state[s % 2, m, pl.ds(pad + start, slab), :]
        copy = copy_of(s, g)
        copy.start()
        return copy

    def merge(s, g):
        state, _, recv, members, first = groups[g]
        _, old_by, new_at, got = plans[s]
        last = s == sections - 1
        for t in range(slots // TILE):
            base = TILE * t - new_at
            window = jnp.clip(base, -TILE, slab) + TILE
            index = row + base
            fresh = (index >= 0) & (index < got)
            filled = row + TILE * t < live
            for m in range(members):
                old = state[s % 2, m, pl.ds(pad + TILE * t + old_by, TILE), :]
                new = recv[s][pl.ds(window + m * slab, TILE), :]
                value = jnp.where(fresh, new, old)
                if last:
                    value = jnp.where(filled, value, 0.0)
                    out_ref[first + m, TILE * t : TILE * t + TILE, :] = value
                else:
                    at = pad + TILE * t
                    state[1 - s % 2, m, at : at + TILE, :] = value

    def merge_leaf(s, leaf):
        _, old_by, new_at, got = plans[s]
        old = pltpu.roll(leaf, lax.rem(slots - old_by, slots), 1)
        new = pltpu.roll(recv_a[s][0:TILE, :], lax.rem(new_at, slots), 1)
        index = lane - new_at
        return jnp.where((index >= 0) & (index < got), new, old)

    loads[0].wait()
    loads[1].wait()
    loads[2].wait()
    pl.semaphore_wait(barrier, sections)

    first = emit(0, 0, leaf)
    second = emit(0, 1, leaf)
    started = []
    for s in range(sections):
        first.wait_recv()
        started += [first, second]
        leaf = merge_leaf(s, leaf)
        merge(s, 0)
        if s + 1 < sections:
            first = emit(s + 1, 0, leaf)
        second.wait_recv()
        merge(s, 1)
        if s + 1 < sections:
            second = emit(s + 1, 1, leaf)
    leaf_out_ref[...] = jnp.where(lane < live, leaf, -1.0)
    for copy in started:
        copy.wait_send()


def moments_kernel(
    max_order,
    depth,
    moved_ref,
    leaf_ref,
    table_ref,
    parity_ref,
    pos_ref,
    chg_ref,
    vel_ref,
    leaves_ref,
    moments_ref,
    parents_ref,
    trans,
    acc,
):
    slots, part = chg_ref.shape
    count = moments_ref.shape[0]
    rows = table_ref.shape[0]
    pos_ref[...] = moved_ref[0:3]
    chg_ref[...] = moved_ref[3]
    vel_ref[...] = moved_ref[4:7]
    found = leaf_ref[0:1, :].astype(jnp.int32)
    leaves_ref[...] = found
    alive = found >= 0
    leaves = jnp.where(alive, found, 0)

    for axis in range(3):
        cell = jnp.zeros_like(leaves)
        for level in range(depth):
            bit = jnp.bitwise_and(jnp.right_shift(leaves, 3 * level + 2 - axis), 1)
            cell = cell + jnp.left_shift(bit, level)
        spots = moved_ref[axis].T
        trans[axis] = 2.0 * (spots * float(2**depth) - cell.astype(jnp.float32)) - 1.0
    trans[3] = moved_ref[3].T

    acc[...] = jnp.zeros_like(acc)
    chunk = 64

    def body(h, carry):
        at = pl.ds(pl.multiple_of(h * chunk, chunk), chunk)
        u = trans[0, at, :]
        v = trans[1, at, :]
        w = trans[2, at, :]
        a = trans[3, at, :]
        k = 0
        for p in range(max_order + 1):
            b = a
            for q in range(max_order + 1 - p):
                d = b
                for r in range(max_order + 1 - p - q):
                    total = d[0:TILE]
                    for n in range(1, chunk // TILE):
                        total = total + d[n * TILE : n * TILE + TILE]
                    acc[k * TILE : k * TILE + TILE, :] += total
                    k += 1
                    if r < max_order - p - q:
                        d = d * w
                if q < max_order - p:
                    b = b * v
            if p < max_order:
                a = a * u
        return carry

    lax.fori_loop(0, part // chunk, body, 0)

    sums = acc[pl.ds(0, rows, stride=TILE), :]
    for n in range(1, TILE):
        sums = sums + acc[pl.ds(n, rows, stride=TILE), :]
    moments = sums * (1.0 / 16.0)
    moments_ref[...] = moments[:count]

    minus = 7 - jnp.bitwise_and(leaves, 7)
    odd = jnp.bitwise_and(parity_ref[...], minus)
    odd = jnp.bitwise_xor(jnp.bitwise_xor(odd, jnp.right_shift(odd, 1)), jnp.right_shift(odd, 2))
    flip = jnp.bitwise_and(odd, 1) == 1

    def dot(table, value, swap):
        parts = []
        rest = value
        for _ in range(3):
            piece = rest.astype(jnp.bfloat16)
            rest = rest - piece.astype(jnp.float32)
            parts.append(piece)
        result = 0.0
        for piece in parts[::-1]:
            left, right = (piece, table) if swap else (table, piece)
            result = result + jnp.dot(left, right, preferred_element_type=jnp.float32)
        return result

    lifted = dot(table_ref[...], jnp.where(flip, -moments, moments), False)
    lifted = jnp.where(flip, -lifted, lifted)
    parent = jnp.right_shift(leaves, 3).astype(jnp.float32)
    across = jnp.broadcast_to(jnp.where(alive, parent, -1.0), (slots, slots))
    down = jnp.broadcast_to(jnp.where(alive, parent, -2.0), (slots, slots)).T
    sibling = (across == down).astype(jnp.bfloat16)
    parents_ref[...] = dot(sibling, lifted, True)[:count]


def per_device(sizes, positions, charges, velocities, leaf_ids, live_counts, send_counts):
    slots, part = charges.shape
    slab = slots // 4
    sections = (sizes[0] * sizes[1] * sizes[2]).bit_length() - 1
    f32 = jnp.float32
    any_space = pl.BlockSpec(memory_space=pl.ANY)
    vmem = pl.BlockSpec(memory_space=pltpu.VMEM)
    smem = pl.BlockSpec(memory_space=pltpu.SMEM)
    rows_a = TILE + 4 * slab
    rows_b = TILE + 3 * slab
    moved, leaf = pl.pallas_call(
        functools.partial(exchange_kernel, sizes),
        out_shape=(
            jax.ShapeDtypeStruct((7, slots, part), f32),
            jax.ShapeDtypeStruct((TILE, slots), f32),
        ),
        in_specs=[smem, smem, vmem, any_space, any_space, any_space],
        out_specs=(vmem, vmem),
        scratch_shapes=[
            pltpu.VMEM((2, 4, slots + 2 * slab, part), f32),
            pltpu.VMEM((2, 3, slots + 2 * slab, part), f32),
            pltpu.VMEM((sections, rows_a, part), f32),
            pltpu.VMEM((sections, rows_b, part), f32),
            pltpu.SemaphoreType.DMA((3,)),
            pltpu.SemaphoreType.DMA((sections, 2)),
            pltpu.SemaphoreType.DMA((sections, 2)),
        ]
        + [pltpu.VMEM((r + TILE, part), f32) for _ in range(sections) for r in (rows_a, rows_b)],
        compiler_params=pltpu.CompilerParams(collective_id=0, has_side_effects=True),
    )(live_counts, send_counts, leaf_ids.reshape(1, slots), positions, charges, velocities)

    count = len(exponents(ORDER))
    rows = -(-count // 16) * 16
    table, parity = shift_constants(ORDER, rows, slots)
    outs = pl.pallas_call(
        functools.partial(moments_kernel, ORDER, LEVEL),
        out_shape=(
            jax.ShapeDtypeStruct(positions.shape, f32),
            jax.ShapeDtypeStruct(charges.shape, f32),
            jax.ShapeDtypeStruct(velocities.shape, f32),
            jax.ShapeDtypeStruct((1, slots), jnp.int32),
            jax.ShapeDtypeStruct((count, slots), f32),
            jax.ShapeDtypeStruct((count, slots), f32),
        ),
        in_specs=[vmem] * 4,
        out_specs=(vmem,) * 6,
        scratch_shapes=[
            pltpu.VMEM((4, part, slots), f32),
            pltpu.VMEM((rows * TILE, slots), f32),
        ],
    )(moved, leaf, table, parity)
    return (outs[0], outs[1], outs[2], outs[3].reshape(slots), outs[4], outs[5])


def solution(mesh):
    sizes = tuple(mesh.shape[name] for name in AXES)
    in_specs = (
        P(None, AXES, None),
        P(AXES, None),
        P(None, AXES, None),
        P(AXES),
        P(),
        P(),
    )
    out_specs = (
        P(None, AXES, None),
        P(AXES, None),
        P(None, AXES, None),
        P(AXES),
        P(None, AXES),
        P(None, AXES),
    )
    return jax.shard_map(
        functools.partial(per_device, sizes),
        mesh=mesh,
        in_specs=in_specs,
        out_specs=out_specs,
        check_vma=False,
    )
```

```python
import functools
import math

import jax
import jax.numpy as jnp
import numpy as np
from jax import lax
from jax.experimental import pallas as pl
from jax.experimental.pallas import tpu as pltpu
from jax.sharding import PartitionSpec as P

ORDER = 10
LEVEL = 7
AXES = ("gx", "gy", "gz")
TILE = 8
MEMBERS = 7
LEAF_CHAIN = 3
CHAIN_ORDER = (3, 0, 1, 2, 4, 5, 6)
SKEW = 3


def exponents(max_order):
    return [
        (p, q, r)
        for p in range(max_order + 1)
        for q in range(max_order + 1 - p)
        for r in range(max_order + 1 - p - q)
    ]


def shift_constants(max_order, rows, lanes):
    triples = exponents(max_order)
    table = np.zeros((rows, rows))
    parity = np.zeros((rows, lanes), np.int32)
    for k, (p, q, r) in enumerate(triples):
        parity[k] = (p & 1) * 4 + (q & 1) * 2 + (r & 1)
        for j, (e, f, g) in enumerate(triples):
            if e <= p and f <= q and g <= r:
                ways = math.comb(p, e) * math.comb(q, f) * math.comb(r, g)
                table[k, j] = ways * 0.5 ** (p + q + r)
    return jnp.asarray(table, jnp.bfloat16), jnp.asarray(parity)


def exchange_kernel(
    sizes,
    live_ref,
    sends_ref,
    leaf_ref,
    pos_ref,
    chg_ref,
    vel_ref,
    out_ref,
    leaf_out_ref,
    slabs,
    in_sem,
    send_sem,
    recv_sem,
    *buffers,
):
    nx, ny, nz = sizes
    sections = (nx * ny * nz).bit_length() - 1
    slots, part = chg_ref.shape
    slab = slots // 4
    pad = slab
    states, arrivals = buffers[:MEMBERS], buffers[MEMBERS:]
    device = (lax.axis_index("gx") * ny + lax.axis_index("gy")) * nz + lax.axis_index("gz")

    sources = [pos_ref.at[0], pos_ref.at[1], pos_ref.at[2], chg_ref]
    sources += [vel_ref.at[0], vel_ref.at[1], vel_ref.at[2]]
    loads = []
    for m in CHAIN_ORDER:
        landing = states[m].at[0, pad : pad + slots, :]
        loads.append(pltpu.make_async_copy(sources[m], landing, in_sem.at[m]))
        loads[-1].start()

    masks = [1 << (sections - 1 - s) for s in range(sections)]
    uppers = [lax.rem(lax.div(device, m), 2) for m in masks]
    partners = [device + m - 2 * m * up for m, up in zip(masks, uppers)]
    places = [
        (lax.div(e, ny * nz), lax.rem(lax.div(e, nz), ny), lax.rem(e, nz)) for e in partners
    ]

    barrier = pltpu.get_barrier_semaphore()
    for place in places:
        pl.semaphore_signal(
            barrier, inc=1, device_id=place, device_id_type=pl.DeviceIdType.MESH
        )

    live = live_ref[device]
    plans = []
    for s in range(sections):
        sent = sends_ref[s, device]
        got = sends_ref[s, partners[s]]
        up = uppers[s]
        kept = live - sent
        start = (1 - up) * kept
        old_by = up * (sent - got)
        plans.append((start, old_by, start, got))
        live = kept + got

    edge = jnp.zeros((pad, part), jnp.float32)
    for m in range(MEMBERS):
        for side in range(2):
            states[m][side, 0:pad, :] = edge
            states[m][side, pad + slots : 2 * pad + slots, :] = edge
    for s in range(sections):
        for m in range(MEMBERS):
            arrived = arrivals[s * MEMBERS + m]
            if m != LEAF_CHAIN:
                arrived[0:TILE, :] = edge[0:TILE]
            arrived[TILE + slab : 2 * TILE + slab, :] = edge[0:TILE]

    lane = lax.broadcasted_iota(jnp.int32, (TILE, slots), 1)
    row = lax.broadcasted_iota(jnp.int32, (TILE, part), 0)

    def emit(s, m, leaf):
        start = plans[s][0]
        first = TILE
        if m == LEAF_CHAIN:
            slabs[s, m, 0:TILE, :] = pltpu.roll(leaf, lax.rem(slots - start, slots), 1)
            first = 0
        slabs[s, m, TILE : TILE + slab, :] = states[m][s % 2, pl.ds(pad + start, slab), :]
        copy = pltpu.make_async_remote_copy(
            src_ref=slabs.at[s, m, first : TILE + slab, :],
            dst_ref=arrivals[s * MEMBERS + m].at[first : TILE + slab, :],
            send_sem=send_sem.at[s, m],
            recv_sem=recv_sem.at[s, m],
            device_id=places[s],
            device_id_type=pl.DeviceIdType.MESH,
        )
        copy.start()
        return copy

    def merge(s, m):
        state, arrived = states[m], arrivals[s * MEMBERS + m]
        _, old_by, new_at, got = plans[s]
        for t in range(slots // TILE):
            base = TILE * t - new_at
            window = jnp.clip(base, -TILE, slab) + TILE
            index = row + base
            fresh = (index >= 0) & (index < got)
            old = state[s % 2, pl.ds(pad + TILE * t + old_by, TILE), :]
            value = jnp.where(fresh, arrived[pl.ds(window, TILE), :], old)
            if s == sections - 1:
                value = jnp.where(row + TILE * t < live, value, 0.0)
                out_ref[m, TILE * t : TILE * t + TILE, :] = value
            else:
                at = pad + TILE * t
                state[1 - s % 2, at : at + TILE, :] = value

    def merge_leaf(s, leaf):
        _, old_by, new_at, got = plans[s]
        old = pltpu.roll(leaf, lax.rem(slots - old_by, slots), 1)
        new = pltpu.roll(arrivals[s * MEMBERS + LEAF_CHAIN][0:TILE, :], lax.rem(new_at, slots), 1)
        index = lane - new_at
        return jnp.where((index >= 0) & (index < got), new, old)

    leaf = jnp.broadcast_to(leaf_ref[...], (TILE, slots)).astype(jnp.float32)
    pl.semaphore_wait(barrier, sections)
    copies = {}
    for n, m in enumerate(CHAIN_ORDER):
        loads[n].wait()
        copies[0, m] = emit(0, m, leaf)
    events = [(SKEW * s + n, s, m) for s in range(sections) for n, m in enumerate(CHAIN_ORDER)]
    for _, s, m in sorted(events):
        copies[s, m].wait_recv()
        if m == LEAF_CHAIN:
            leaf = merge_leaf(s, leaf)
        merge(s, m)
        if s + 1 < sections:
            copies[s + 1, m] = emit(s + 1, m, leaf)
    leaf_out_ref[...] = jnp.where(lane < live, leaf, -1.0)
    for copy in copies.values():
        copy.wait_send()


def moments_kernel(
    max_order,
    depth,
    moved_ref,
    leaf_ref,
    table_ref,
    parity_ref,
    pos_ref,
    chg_ref,
    vel_ref,
    leaves_ref,
    moments_ref,
    parents_ref,
    trans,
    acc,
):
    slots, part = chg_ref.shape
    count = moments_ref.shape[0]
    rows = table_ref.shape[0]
    pos_ref[...] = moved_ref[0:3]
    chg_ref[...] = moved_ref[3]
    vel_ref[...] = moved_ref[4:7]
    found = leaf_ref[0:1, :].astype(jnp.int32)
    leaves_ref[...] = found
    alive = found >= 0
    leaves = jnp.where(alive, found, 0)

    for axis in range(3):
        cell = jnp.zeros_like(leaves)
        for level in range(depth):
            bit = jnp.bitwise_and(jnp.right_shift(leaves, 3 * level + 2 - axis), 1)
            cell = cell + jnp.left_shift(bit, level)
        spots = moved_ref[axis].T
        trans[axis] = 2.0 * (spots * float(2**depth) - cell.astype(jnp.float32)) - 1.0
    trans[3] = moved_ref[3].T

    acc[...] = jnp.zeros_like(acc)
    chunk = 64

    def body(h, carry):
        at = pl.ds(pl.multiple_of(h * chunk, chunk), chunk)
        u = trans[0, at, :]
        v = trans[1, at, :]
        w = trans[2, at, :]
        a = trans[3, at, :]
        k = 0
        for p in range(max_order + 1):
            b = a
            for q in range(max_order + 1 - p):
                d = b
                for r in range(max_order + 1 - p - q):
                    total = d[0:TILE]
                    for n in range(1, chunk // TILE):
                        total = total + d[n * TILE : n * TILE + TILE]
                    acc[k * TILE : k * TILE + TILE, :] += total
                    k += 1
                    if r < max_order - p - q:
                        d = d * w
                if q < max_order - p:
                    b = b * v
            if p < max_order:
                a = a * u
        return carry

    lax.fori_loop(0, part // chunk, body, 0)

    sums = acc[pl.ds(0, rows, stride=TILE), :]
    for n in range(1, TILE):
        sums = sums + acc[pl.ds(n, rows, stride=TILE), :]
    moments = sums * (1.0 / 16.0)
    moments_ref[...] = moments[:count]

    minus = 7 - jnp.bitwise_and(leaves, 7)
    odd = jnp.bitwise_and(parity_ref[...], minus)
    odd = jnp.bitwise_xor(jnp.bitwise_xor(odd, jnp.right_shift(odd, 1)), jnp.right_shift(odd, 2))
    flip = jnp.bitwise_and(odd, 1) == 1

    def dot(table, value, swap):
        parts = []
        rest = value
        for _ in range(3):
            piece = rest.astype(jnp.bfloat16)
            rest = rest - piece.astype(jnp.float32)
            parts.append(piece)
        result = 0.0
        for piece in parts[::-1]:
            left, right = (piece, table) if swap else (table, piece)
            result = result + jnp.dot(left, right, preferred_element_type=jnp.float32)
        return result

    lifted = dot(table_ref[...], jnp.where(flip, -moments, moments), False)
    lifted = jnp.where(flip, -lifted, lifted)
    parent = jnp.right_shift(leaves, 3).astype(jnp.float32)
    across = jnp.broadcast_to(jnp.where(alive, parent, -1.0), (slots, slots))
    down = jnp.broadcast_to(jnp.where(alive, parent, -2.0), (slots, slots)).T
    sibling = (across == down).astype(jnp.bfloat16)
    parents_ref[...] = dot(sibling, lifted, True)[:count]


def per_device(sizes, positions, charges, velocities, leaf_ids, live_counts, send_counts):
    slots, part = charges.shape
    slab = slots // 4
    sections = (sizes[0] * sizes[1] * sizes[2]).bit_length() - 1
    f32 = jnp.float32
    any_space = pl.BlockSpec(memory_space=pl.ANY)
    vmem = pl.BlockSpec(memory_space=pltpu.VMEM)
    smem = pl.BlockSpec(memory_space=pltpu.SMEM)
    moved, leaf = pl.pallas_call(
        functools.partial(exchange_kernel, sizes),
        out_shape=(
            jax.ShapeDtypeStruct((MEMBERS, slots, part), f32),
            jax.ShapeDtypeStruct((TILE, slots), f32),
        ),
        in_specs=[smem, smem, vmem, any_space, any_space, any_space],
        out_specs=(vmem, vmem),
        scratch_shapes=[
            pltpu.VMEM((sections, MEMBERS, TILE + slab, part), f32),
            pltpu.SemaphoreType.DMA((MEMBERS,)),
            pltpu.SemaphoreType.DMA((sections, MEMBERS)),
            pltpu.SemaphoreType.DMA((sections, MEMBERS)),
        ]
        + [pltpu.VMEM((2, slots + 2 * slab, part), f32)] * MEMBERS
        + [pltpu.VMEM((slab + 2 * TILE, part), f32)] * (sections * MEMBERS),
        compiler_params=pltpu.CompilerParams(collective_id=0, has_side_effects=True),
    )(live_counts, send_counts, leaf_ids.reshape(1, slots), positions, charges, velocities)

    count = len(exponents(ORDER))
    rows = -(-count // 16) * 16
    table, parity = shift_constants(ORDER, rows, slots)
    outs = pl.pallas_call(
        functools.partial(moments_kernel, ORDER, LEVEL),
        out_shape=(
            jax.ShapeDtypeStruct(positions.shape, f32),
            jax.ShapeDtypeStruct(charges.shape, f32),
            jax.ShapeDtypeStruct(velocities.shape, f32),
            jax.ShapeDtypeStruct((1, slots), jnp.int32),
            jax.ShapeDtypeStruct((count, slots), f32),
            jax.ShapeDtypeStruct((count, slots), f32),
        ),
        in_specs=[vmem] * 4,
        out_specs=(vmem,) * 6,
        scratch_shapes=[
            pltpu.VMEM((4, part, slots), f32),
            pltpu.VMEM((rows * TILE, slots), f32),
        ],
    )(moved, leaf, table, parity)
    return (outs[0], outs[1], outs[2], outs[3].reshape(slots), outs[4], outs[5])


def solution(mesh):
    sizes = tuple(mesh.shape[name] for name in AXES)
    in_specs = (
        P(None, AXES, None),
        P(AXES, None),
        P(None, AXES, None),
        P(AXES),
        P(),
        P(),
    )
    out_specs = (
        P(None, AXES, None),
        P(AXES, None),
        P(None, AXES, None),
        P(AXES),
        P(None, AXES),
        P(None, AXES),
    )
    return jax.shard_map(
        functools.partial(per_device, sizes),
        mesh=mesh,
        in_specs=in_specs,
        out_specs=out_specs,
        check_vma=False,
    )
```

```python
import functools
import math

import jax
import jax.numpy as jnp
import numpy as np
from jax import lax
from jax.experimental import pallas as pl
from jax.experimental.pallas import tpu as pltpu
from jax.sharding import PartitionSpec as P

ORDER = 10
LEVEL = 7
AXES = ("gx", "gy", "gz")
TILE = 8
MEMBERS = 7
LEAF_CHAIN = 3
CHAIN_ORDER = (3, 0, 1, 2, 4, 5, 6)


def exponents(max_order):
    return [
        (p, q, r)
        for p in range(max_order + 1)
        for q in range(max_order + 1 - p)
        for r in range(max_order + 1 - p - q)
    ]


def shift_constants(max_order, rows, lanes):
    triples = exponents(max_order)
    table = np.zeros((rows, rows))
    parity = np.zeros((rows, lanes), np.int32)
    for k, (p, q, r) in enumerate(triples):
        parity[k] = (p & 1) * 4 + (q & 1) * 2 + (r & 1)
        for j, (e, f, g) in enumerate(triples):
            if e <= p and f <= q and g <= r:
                ways = math.comb(p, e) * math.comb(q, f) * math.comb(r, g)
                table[k, j] = ways * 0.5 ** (p + q + r)
    return jnp.asarray(table, jnp.bfloat16), jnp.asarray(parity)


def exchange_kernel(
    sizes,
    live_ref,
    sends_ref,
    leaf_ref,
    pos_ref,
    chg_ref,
    vel_ref,
    out_ref,
    leaf_out_ref,
    slabs,
    result,
    in_sem,
    out_sem,
    send_sem,
    recv_sem,
    *buffers,
):
    nx, ny, nz = sizes
    sections = (nx * ny * nz).bit_length() - 1
    slots, part = chg_ref.shape
    slab = slots // 4
    pad = slab
    states, arrivals = buffers[:MEMBERS], buffers[MEMBERS:]
    device = (lax.axis_index("gx") * ny + lax.axis_index("gy")) * nz + lax.axis_index("gz")

    sources = [pos_ref.at[0], pos_ref.at[1], pos_ref.at[2], chg_ref]
    sources += [vel_ref.at[0], vel_ref.at[1], vel_ref.at[2]]
    loads = []
    for m in CHAIN_ORDER:
        landing = states[m].at[0, pad : pad + slots, :]
        loads.append(pltpu.make_async_copy(sources[m], landing, in_sem.at[m]))
        loads[-1].start()

    masks = [1 << (sections - 1 - s) for s in range(sections)]
    uppers = [lax.rem(lax.div(device, m), 2) for m in masks]
    partners = [device + m - 2 * m * up for m, up in zip(masks, uppers)]
    places = [
        (lax.div(e, ny * nz), lax.rem(lax.div(e, nz), ny), lax.rem(e, nz)) for e in partners
    ]

    barrier = pltpu.get_barrier_semaphore()
    for place in places:
        pl.semaphore_signal(
            barrier, inc=1, device_id=place, device_id_type=pl.DeviceIdType.MESH
        )

    live = live_ref[device]
    plans = []
    for s in range(sections):
        sent = sends_ref[s, device]
        got = sends_ref[s, partners[s]]
        up = uppers[s]
        kept = live - sent
        start = (1 - up) * kept
        old_by = up * (sent - got)
        plans.append((start, old_by, start, got))
        live = kept + got

    edge = jnp.zeros((pad, part), jnp.float32)
    for m in range(MEMBERS):
        for side in range(2):
            states[m][side, 0:pad, :] = edge
            states[m][side, pad + slots : 2 * pad + slots, :] = edge
    for s in range(sections):
        for m in range(MEMBERS):
            arrived = arrivals[s * MEMBERS + m]
            if m != LEAF_CHAIN:
                arrived[0:TILE, :] = edge[0:TILE]
            arrived[TILE + slab : 2 * TILE + slab, :] = edge[0:TILE]

    lane = lax.broadcasted_iota(jnp.int32, (TILE, slots), 1)
    row = lax.broadcasted_iota(jnp.int32, (TILE, part), 0)

    def joined(s, m, first):
        state, arrived = states[m], arrivals[s * MEMBERS + m]
        _, old_by, new_at, got = plans[s]
        base = first - new_at
        index = row + base
        fresh = (index >= 0) & (index < got)
        window = jnp.clip(base, -TILE, slab) + TILE
        place = jnp.minimum(pad + first + old_by, 2 * pad + slots - TILE)
        return jnp.where(
            fresh, arrived[pl.ds(window, TILE), :], state[s % 2, pl.ds(place, TILE), :]
        )

    def emit(s, m, leaf):
        start = plans[s][0]
        first = TILE
        if m == LEAF_CHAIN:
            slabs[s, m, 0:TILE, :] = pltpu.roll(leaf, lax.rem(slots - start, slots), 1)
            first = 0
        for t in range(slab // TILE):
            at = TILE * t
            if s == 0:
                value = states[m][0, pl.ds(pad + start + at, TILE), :]
            else:
                value = joined(s - 1, m, start + at)
            slabs[s, m, TILE + at : 2 * TILE + at, :] = value
        copy = pltpu.make_async_remote_copy(
            src_ref=slabs.at[s, m, first : TILE + slab, :],
            dst_ref=arrivals[s * MEMBERS + m].at[first : TILE + slab, :],
            send_sem=send_sem.at[s, m],
            recv_sem=recv_sem.at[s, m],
            device_id=places[s],
            device_id_type=pl.DeviceIdType.MESH,
        )
        copy.start()
        return copy

    def merge(s, m):
        for t in range(slots // TILE):
            at = TILE * t
            value = joined(s, m, at)
            if s == sections - 1:
                value = jnp.where(row + at < live, value, 0.0)
                result[m, at : at + TILE, :] = value
            else:
                states[m][1 - s % 2, pad + at : pad + at + TILE, :] = value

    def shifted_leaf(s, leaf):
        return pltpu.roll(leaf, lax.rem(slots - plans[s][1], slots), 1)

    def merge_leaf(s, old):
        _, _, new_at, got = plans[s]
        new = pltpu.roll(arrivals[s * MEMBERS + LEAF_CHAIN][0:TILE, :], lax.rem(new_at, slots), 1)
        index = lane - new_at
        return jnp.where((index >= 0) & (index < got), new, old)

    leaf = jnp.broadcast_to(leaf_ref[...], (TILE, slots)).astype(jnp.float32)
    pl.semaphore_wait(barrier, sections)
    copies = {}
    for n, m in enumerate(CHAIN_ORDER):
        loads[n].wait()
        copies[0, m] = emit(0, m, leaf)
    stores = []
    for s in range(sections):
        old_leaf = shifted_leaf(s, leaf)
        for m in CHAIN_ORDER:
            copies[s, m].wait_recv()
            if m == LEAF_CHAIN:
                leaf = merge_leaf(s, old_leaf)
            if s + 1 < sections:
                copies[s + 1, m] = emit(s + 1, m, leaf)
            else:
                merge(s, m)
                stores.append(pltpu.make_async_copy(result.at[m], out_ref.at[m], out_sem.at[m]))
                stores[-1].start()
        if s + 1 < sections:
            for m in CHAIN_ORDER:
                merge(s, m)
    leaf_out_ref[...] = jnp.where(lane < live, leaf, -1.0)
    for copy in copies.values():
        copy.wait_send()
    for store in stores:
        store.wait()


def moments_kernel(
    max_order,
    depth,
    moved_ref,
    leaf_ref,
    table_ref,
    parity_ref,
    pos_ref,
    chg_ref,
    vel_ref,
    leaves_ref,
    moments_ref,
    parents_ref,
    trans,
    acc,
):
    slots, part = chg_ref.shape
    count = moments_ref.shape[0]
    rows = table_ref.shape[0]
    pos_ref[...] = moved_ref[0:3]
    chg_ref[...] = moved_ref[3]
    vel_ref[...] = moved_ref[4:7]
    found = leaf_ref[0:1, :].astype(jnp.int32)
    leaves_ref[...] = found
    alive = found >= 0
    leaves = jnp.where(alive, found, 0)

    for axis in range(3):
        cell = jnp.zeros_like(leaves)
        for level in range(depth):
            bit = jnp.bitwise_and(jnp.right_shift(leaves, 3 * level + 2 - axis), 1)
            cell = cell + jnp.left_shift(bit, level)
        spots = moved_ref[axis].T
        trans[axis] = 2.0 * (spots * float(2**depth) - cell.astype(jnp.float32)) - 1.0
    trans[3] = moved_ref[3].T

    acc[...] = jnp.zeros_like(acc)
    chunk = 64

    def body(h, carry):
        at = pl.ds(pl.multiple_of(h * chunk, chunk), chunk)
        u = trans[0, at, :]
        v = trans[1, at, :]
        w = trans[2, at, :]
        a = trans[3, at, :]
        k = 0
        for p in range(max_order + 1):
            b = a
            for q in range(max_order + 1 - p):
                d = b
                for r in range(max_order + 1 - p - q):
                    total = d[0:TILE]
                    for n in range(1, chunk // TILE):
                        total = total + d[n * TILE : n * TILE + TILE]
                    acc[k * TILE : k * TILE + TILE, :] += total
                    k += 1
                    if r < max_order - p - q:
                        d = d * w
                if q < max_order - p:
                    b = b * v
            if p < max_order:
                a = a * u
        return carry

    lax.fori_loop(0, part // chunk, body, 0)

    sums = acc[pl.ds(0, rows, stride=TILE), :]
    for n in range(1, TILE):
        sums = sums + acc[pl.ds(n, rows, stride=TILE), :]
    moments = sums * (1.0 / 16.0)
    moments_ref[...] = moments[:count]

    minus = 7 - jnp.bitwise_and(leaves, 7)
    odd = jnp.bitwise_and(parity_ref[...], minus)
    odd = jnp.bitwise_xor(jnp.bitwise_xor(odd, jnp.right_shift(odd, 1)), jnp.right_shift(odd, 2))
    flip = jnp.bitwise_and(odd, 1) == 1

    def dot(table, value, swap):
        parts = []
        rest = value
        for _ in range(3):
            piece = rest.astype(jnp.bfloat16)
            rest = rest - piece.astype(jnp.float32)
            parts.append(piece)
        result = 0.0
        for piece in parts[::-1]:
            left, right = (piece, table) if swap else (table, piece)
            result = result + jnp.dot(left, right, preferred_element_type=jnp.float32)
        return result

    lifted = dot(table_ref[...], jnp.where(flip, -moments, moments), False)
    lifted = jnp.where(flip, -lifted, lifted)
    parent = jnp.right_shift(leaves, 3).astype(jnp.float32)
    across = jnp.broadcast_to(jnp.where(alive, parent, -1.0), (slots, slots))
    down = jnp.broadcast_to(jnp.where(alive, parent, -2.0), (slots, slots)).T
    sibling = (across == down).astype(jnp.bfloat16)
    parents_ref[...] = dot(sibling, lifted, True)[:count]


def per_device(sizes, positions, charges, velocities, leaf_ids, live_counts, send_counts):
    slots, part = charges.shape
    slab = slots // 4
    sections = (sizes[0] * sizes[1] * sizes[2]).bit_length() - 1
    f32 = jnp.float32
    any_space = pl.BlockSpec(memory_space=pl.ANY)
    vmem = pl.BlockSpec(memory_space=pltpu.VMEM)
    smem = pl.BlockSpec(memory_space=pltpu.SMEM)
    moved, leaf = pl.pallas_call(
        functools.partial(exchange_kernel, sizes),
        out_shape=(
            jax.ShapeDtypeStruct((MEMBERS, slots, part), f32),
            jax.ShapeDtypeStruct((TILE, slots), f32),
        ),
        in_specs=[smem, smem, vmem, any_space, any_space, any_space],
        out_specs=(any_space, vmem),
        scratch_shapes=[
            pltpu.VMEM((sections, MEMBERS, TILE + slab, part), f32),
            pltpu.VMEM((MEMBERS, slots, part), f32),
            pltpu.SemaphoreType.DMA((MEMBERS,)),
            pltpu.SemaphoreType.DMA((MEMBERS,)),
            pltpu.SemaphoreType.DMA((sections, MEMBERS)),
            pltpu.SemaphoreType.DMA((sections, MEMBERS)),
        ]
        + [pltpu.VMEM((2, slots + 2 * slab, part), f32)] * MEMBERS
        + [pltpu.VMEM((slab + 2 * TILE, part), f32)] * (sections * MEMBERS),
        compiler_params=pltpu.CompilerParams(collective_id=0, has_side_effects=True),
    )(live_counts, send_counts, leaf_ids.reshape(1, slots), positions, charges, velocities)

    count = len(exponents(ORDER))
    rows = -(-count // 16) * 16
    table, parity = shift_constants(ORDER, rows, slots)
    outs = pl.pallas_call(
        functools.partial(moments_kernel, ORDER, LEVEL),
        out_shape=(
            jax.ShapeDtypeStruct(positions.shape, f32),
            jax.ShapeDtypeStruct(charges.shape, f32),
            jax.ShapeDtypeStruct(velocities.shape, f32),
            jax.ShapeDtypeStruct((1, slots), jnp.int32),
            jax.ShapeDtypeStruct((count, slots), f32),
            jax.ShapeDtypeStruct((count, slots), f32),
        ),
        in_specs=[vmem] * 4,
        out_specs=(vmem,) * 6,
        scratch_shapes=[
            pltpu.VMEM((4, part, slots), f32),
            pltpu.VMEM((rows * TILE, slots), f32),
        ],
    )(moved, leaf, table, parity)
    return (outs[0], outs[1], outs[2], outs[3].reshape(slots), outs[4], outs[5])


def solution(mesh):
    sizes = tuple(mesh.shape[name] for name in AXES)
    in_specs = (
        P(None, AXES, None),
        P(AXES, None),
        P(None, AXES, None),
        P(AXES),
        P(),
        P(),
    )
    out_specs = (
        P(None, AXES, None),
        P(AXES, None),
        P(None, AXES, None),
        P(AXES),
        P(None, AXES),
        P(None, AXES),
    )
    return jax.shard_map(
        functools.partial(per_device, sizes),
        mesh=mesh,
        in_specs=in_specs,
        out_specs=out_specs,
        check_vma=False,
    )
```
